32 devices in a mesh: samp: 4 (over x, core), snp: 8 (over z, y).
Axes of the slice: x: 2, y: 2, z: 4, core: 2. Of those that a mesh axis runs over, the one named last changes fastest.
Arguments:
- genotypes: float32 [4096, 8192], P('samp', 'snp'), may hold values from -1 to 2, as said below
Outputs:
- band_r: float32 [8192, 4096], P('snp', 'samp')
The draws below stay inside these ranges and needn't reach their ends.
Inputs may be any that keep to these rules, and one draw needn't show every extreme that they name: `genotypes`: -1 marks a missing dosage; every other value lies between 0 and 2. Every eighth sample (samples 0, 8, 16, ...) has no missing dosage, and over those samples each SNP's dosages run through 0, 1, 2 cyclically from a SNP's own starting value.
All inputs are finite; a program needn't handle non-finite values.
Results may differ from the reference program's by a relative error of at most 0.006.
Values may be sent and summed in bfloat16 or wider, within the bound.
No kernel may reach another device: no remote copies, remote signals or barrier semaphores. Data moves between devices by JAX's collectives and lax.ppermute only.
A program may use at most 64 MiB of HBM per device.

```python
import jax
import jax.numpy as jnp
from jax import lax

TILE = 512
BAND = 4096
NSAMP = 4096
NSNP = 8192


def draw_genotypes(key, part):
    window = 32
    key_bits = jax.random.fold_in(key, 11)
    key_offset = jax.random.fold_in(key, 12)
    key_cycle = jax.random.fold_in(key, 13)
    key_missing = jax.random.fold_in(key, 14)
    key_jitter = jax.random.fold_in(key, 15)
    bits = jax.random.randint(key_bits, (NSAMP, NSNP + window), 0, 2, dtype=jnp.int32)
    running = jnp.cumsum(bits, axis=1)
    window_sum = running[:, window:] - running[:, :-window]
    offset = jax.random.randint(key_offset, (NSNP,), -4, 5, dtype=jnp.int32)
    sample_row = jnp.arange(NSAMP, dtype=jnp.int32)
    drift = 6 * sample_row // NSAMP
    level = (window_sum + offset[None, :] + drift[:, None]).astype(jnp.float32)
    jitter = jax.random.uniform(key_jitter, (NSAMP, NSNP), jnp.float32, 0.0, 1.0)
    temper = 2.0
    dosage = 2.0 * jax.nn.sigmoid((level + jitter - 19.0) / temper)
    cycle_start = jax.random.randint(key_cycle, (NSNP,), 0, 3, dtype=jnp.int32)
    anchor = (sample_row % 8 == 0)[:, None]
    cycled = ((sample_row[:, None] // 8 + cycle_start[None, :]) % 3).astype(jnp.float32)
    dosage = jnp.where(anchor, cycled, dosage)
    percent = 3 + 9 * sample_row // NSAMP
    missing_roll = jax.random.randint(key_missing, (NSAMP, NSNP), 0, 100, dtype=jnp.int32)
    missing = (missing_roll < percent[:, None]) & jnp.logical_not(anchor)
    return jnp.where(missing, -1.0, dosage).astype(jnp.float32)


def setup_inputs(seed: int = 0) -> dict:
    splits = jax.random.split(jax.random.key(seed), 2)
    genotypes = draw_genotypes(jax.random.fold_in(splits[1], 71), 0)
    return dict(genotypes=genotypes)


EPS = 1e-05

def reference(genotypes):
    present = (genotypes >= 0).astype(jnp.float32)
    dosage = genotypes.astype(jnp.float32) * present
    counted = lax.optimization_barrier(jnp.sum(present, axis=0))
    summed = lax.optimization_barrier(jnp.sum(dosage, axis=0))
    squared = lax.optimization_barrier(jnp.sum(dosage * dosage, axis=0))
    average = summed / counted
    spread = squared / counted - average * average
    scaled = (present * (dosage - average) * lax.rsqrt(spread + EPS)).astype(jnp.bfloat16)
    col_norms = counted * spread / (spread + EPS)
    total_snps = genotypes.shape[1]
    padded = jnp.concatenate([scaled, jnp.zeros((scaled.shape[0], BAND), scaled.dtype)], axis=1)
    padded_norms = jnp.concatenate([col_norms, jnp.ones((BAND,), jnp.float32)])

    def band_tile(tile_pos):
        start = (tile_pos * TILE).astype(jnp.int32)
        row_block = lax.dynamic_slice_in_dim(scaled, start, TILE, 1)
        col_block = lax.dynamic_slice_in_dim(padded, start, BAND, 1)
        products = lax.dot_general(row_block, col_block, (((0,), (0,)), ((), ())), preferred_element_type=jnp.float32)
        row_norm = lax.dynamic_slice_in_dim(col_norms, start, TILE, 0)
        col_norm = lax.dynamic_slice_in_dim(padded_norms, start, BAND, 0)
        return products / jnp.sqrt(row_norm[:, None] * col_norm[None, :])
    tiles = lax.map(band_tile, jnp.arange(total_snps // TILE, dtype=jnp.int32))
    return tiles.reshape(total_snps, BAND)
```

```python
import jax
import jax.numpy as jnp
from jax import lax
from jax.experimental import pallas as pl
from jax.experimental.pallas import tpu as pltpu
from jax.sharding import PartitionSpec as P

TILE = 512
BAND = 4096
CHUNKS = 4


def dot_t(rows, cols):
    return lax.dot_general(rows, cols, (((0,), (0,)), ((), ())), preferred_element_type=jnp.float32)


def make_on_device(samp_size, snp_size):
    axes = ("samp", "snp")

    def perm(x, move):
        pairs = []
        for samp in range(samp_size):
            for p in range(snp_size):
                target = move(samp // 2, samp % 2, p)
                if target is None:
                    continue
                tx, tc, tp = target
                if 0 <= tp < snp_size:
                    pairs.append((samp * snp_size + p, (tx * 2 + tc) * snp_size + tp))
        return lax.ppermute(x, axes, pairs)

    def core_swap(x):
        return perm(x, lambda xx, c, p: (xx, 1 - c, p))

    def x_swap(x):
        return perm(x, lambda xx, c, p: (1 - xx, c, p))

    def standardize_body(core_ref, stat_ref, own_ref, other_ref, whole_ref, *chunk_refs):
        counted = stat_ref[0:1, :]
        summed = stat_ref[1:2, :]
        squared = stat_ref[2:3, :]
        average = summed / counted
        spread = squared / counted - average * average
        factor = lax.rsqrt(counted * spread)
        for half, ref in enumerate((own_ref, other_ref)):
            g = ref[...]
            u = jnp.where(g >= 0, (g - average) * factor, 0.0).astype(jnp.bfloat16)
            whole_ref[half] = u
        width = chunk_refs[0].shape[2]
        for j, ref in enumerate(chunk_refs):
            start = pl.multiple_of(core_ref[0] * TILE + j * width, width)
            ref[...] = whole_ref[:, :, pl.ds(start, width)]

    def standardize(core, stats, own, other):
        samples, snps = own.shape
        block = samples // 8
        width = TILE // CHUNKS
        return pl.pallas_call(
            standardize_body,
            grid_spec=pltpu.PrefetchScalarGridSpec(
                num_scalar_prefetch=1,
                grid=(samples // block,),
                in_specs=[
                    pl.BlockSpec((3, snps), lambda i, c: (0, 0)),
                    pl.BlockSpec((block, snps), lambda i, c: (i, 0)),
                    pl.BlockSpec((block, snps), lambda i, c: (i, 0)),
                ],
                out_specs=[pl.BlockSpec((2, block, snps), lambda i, c: (0, i, 0))]
                + [pl.BlockSpec((2, block, width), lambda i, c: (0, i, 0))] * CHUNKS,
            ),
            out_shape=[jax.ShapeDtypeStruct((2, samples, snps), jnp.bfloat16)]
            + [jax.ShapeDtypeStruct((2, samples, width), jnp.bfloat16)] * CHUNKS,
            cost_estimate=pl.CostEstimate(flops=8 * samples * snps, bytes_accessed=14 * samples * snps, transcendentals=0),
        )(core, stats, own, other)

    def on_device(genotypes):
        samples, snps = genotypes.shape
        assert samp_size == 4 and snp_size % 2 == 0
        assert snps == 2 * TILE and BAND == 4 * snps
        bf16 = jnp.bfloat16
        samp = lax.axis_index("samp")
        xx, core = samp // 2, samp % 2
        p = lax.axis_index("snp")
        even = (p % 2) == 0
        first_core = core == 0

        other = core_swap(genotypes)
        present = (genotypes >= 0).astype(jnp.float32)
        dosage = genotypes * present
        stats = jnp.stack([jnp.sum(present, axis=0), jnp.sum(dosage, axis=0), jnp.sum(dosage * dosage, axis=0)])
        stats = stats + core_swap(stats)
        stats = stats + x_swap(stats)
        whole, *chunks = standardize(core[None].astype(jnp.int32), stats, genotypes, other)
        whole = whole.reshape(2 * samples, snps)
        chunks = [c.reshape(2 * samples, -1) for c in chunks]

        above = [perm(c, lambda xx, c, p: (xx, c, p - 2)) for c in chunks]
        half = CHUNKS // 2
        up = [
            perm(jnp.concatenate(chunks[i : i + half], axis=1), lambda xx, c, p: (xx, c, p + 2))
            for i in (0, half)
        ]
        nexts = [
            perm(jnp.where(even, a, c), lambda xx, c, p: (xx, c, p + 1 - 2 * (p % 2))) for a, c in zip(above, chunks)
        ]
        up_other = [core_swap(jnp.concatenate([u[samples:], u[:samples]], axis=0)) for u in up]
        mine = jnp.concatenate(up, axis=1)
        theirs = jnp.concatenate(up_other, axis=1)
        below = jnp.concatenate(
            [jnp.where(first_core, mine, theirs), jnp.where(first_core, theirs, mine)], axis=1
        )

        d0 = dot_t(whole, jnp.concatenate(chunks, axis=1))
        d1 = [dot_t(whole, n) for n in nexts]
        d2 = jnp.concatenate([dot_t(whole, a) for a in above], axis=1)
        d3 = [dot_t(below, n).astype(bf16) for n in nexts]
        d4 = jnp.concatenate([dot_t(below[:, TILE:], a).astype(bf16) for a in above], axis=1)

        z_near, z_far = [], []
        for i in (0, half):
            part = jnp.concatenate(d3[i : i + half], axis=1)
            z_near.append(perm(part, lambda xx, c, p: (1, c, p - 2) if xx == 1 else None))
            z_far.append(perm(part, lambda xx, c, p: (1, c, p - 2) if xx == 0 else None))
        q_near = perm(d4, lambda xx, c, p: (1, 1, p - 2) if (xx, c) == (1, 0) else None)
        q_far = perm(d4, lambda xx, c, p: (1, 1, p - 2) if (xx, c) == (0, 0) else None)

        def to_first(x):
            return perm(x, lambda xx, c, p: (0, c, p) if xx == 1 else None)

        x_d0_top = to_first(d0[:TILE].astype(bf16))
        x_d0_low = perm(d0[TILE:].astype(bf16), lambda xx, c, p: (0, c, p) if (xx, c) == (1, 1) else None)
        x_d1 = [to_first(jnp.concatenate(d1[i : i + half], axis=1).astype(bf16)) for i in (0, half)]
        x_d2_top = perm(d2[:TILE].astype(bf16), lambda xx, c, p: (1, c, p) if xx == 0 else None)
        x_d2_low = perm(
            d2[TILE:].astype(bf16), lambda xx, c, p: (1 - xx, c, p) if (xx, c) in ((1, 0), (0, 1)) else None
        )
        f32 = jnp.float32
        d0_top = d0[:TILE] + x_d0_top.astype(f32)
        d0_low = d0[TILE:] + x_d0_low.astype(f32)
        d1 = jnp.concatenate(d1, axis=1) + jnp.concatenate(x_d1, axis=1).astype(f32)
        d2_top = d2[:TILE] + x_d2_top.astype(f32)
        d2_low = d2[TILE:] + x_d2_low.astype(f32)
        d3 = jnp.concatenate(z_near, axis=1).astype(f32) + jnp.concatenate(z_far, axis=1).astype(f32)
        d4 = q_near.astype(f32) + q_far.astype(f32)

        x_first = xx == 0
        send_top = jnp.where(x_first, jnp.where(first_core, d1[:TILE], d0_top), jnp.where(first_core, d3[:TILE], d2_top))
        send_low = jnp.where(first_core, jnp.where(x_first, d2_low, 0.0), jnp.where(x_first, d0_low, d2_low))
        got = core_swap(jnp.concatenate([send_top, send_low], axis=0).astype(bf16)).astype(f32)
        own_top = jnp.where(x_first, jnp.where(first_core, d0_top, d1[:TILE]), jnp.where(first_core, d2_top, d3[:TILE]))
        own_low = jnp.where(x_first, d1[TILE:], d3[TILE:])
        got_top = got[:TILE]
        got_low = got[TILE:] + d4
        top = jnp.concatenate(
            [jnp.where(first_core, own_top, got_top), jnp.where(first_core, got_top, own_top)], axis=1
        )
        low = jnp.concatenate(
            [jnp.where(first_core, got_low, own_low), jnp.where(first_core, own_low, got_low)], axis=1
        )
        return jnp.concatenate([top, low], axis=0)

    return on_device


def solution(mesh):
    body = make_on_device(mesh.shape["samp"], mesh.shape["snp"])
    return jax.shard_map(
        body, mesh=mesh, in_specs=(P("samp", "snp"),), out_specs=P("snp", "samp"), check_vma=False
    )
```

```python
import jax
import jax.numpy as jnp
from jax import lax
from jax.experimental import pallas as pl
from jax.experimental.pallas import tpu as pltpu
from jax.sharding import PartitionSpec as P

TILE = 512
BAND = 4096
CHUNKS = 2


def dot_t(rows, cols):
    return lax.dot_general(rows, cols, (((0,), (0,)), ((), ())), preferred_element_type=jnp.float32)


def dot_pair(rows, cols):
    return dot_t(rows[0], cols[0]) + dot_t(rows[1], cols[1])


def standardize_body(core_ref, stat_ref, own_ref, whole_ref, *chunk_refs):
    counted = stat_ref[0:1, :]
    summed = stat_ref[1:2, :]
    squared = stat_ref[2:3, :]
    average = summed / counted
    spread = squared / counted - average * average
    factor = lax.rsqrt(counted * spread)
    g = own_ref[...]
    whole_ref[...] = jnp.where(g >= 0, (g - average) * factor, 0.0).astype(jnp.bfloat16)
    width = chunk_refs[0].shape[1]
    for k, ref in enumerate(chunk_refs):
        tile = core_ref[0] if k < CHUNKS else 1 - core_ref[0]
        start = pl.multiple_of(tile * TILE + (k % CHUNKS) * width, width)
        ref[...] = whole_ref[:, pl.ds(start, width)]


def standardize(core, stats, own):
    samples, snps = own.shape
    block = samples // 8
    width = TILE // CHUNKS
    out = pl.pallas_call(
        standardize_body,
        grid_spec=pltpu.PrefetchScalarGridSpec(
            num_scalar_prefetch=1,
            grid=(samples // block,),
            in_specs=[
                pl.BlockSpec((3, snps), lambda i, c: (0, 0)),
                pl.BlockSpec((block, snps), lambda i, c: (i, 0)),
            ],
            out_specs=[pl.BlockSpec((block, snps), lambda i, c: (i, 0))]
            + [pl.BlockSpec((block, width), lambda i, c: (i, 0))] * (2 * CHUNKS),
        ),
        out_shape=[jax.ShapeDtypeStruct((samples, snps), jnp.bfloat16)]
        + [jax.ShapeDtypeStruct((samples, width), jnp.bfloat16)] * (2 * CHUNKS),
        cost_estimate=pl.CostEstimate(flops=8 * samples * snps, bytes_accessed=8 * samples * snps, transcendentals=0),
    )(core, stats, own)
    return out[0], out[1 : 1 + CHUNKS], out[1 + CHUNKS :]


def make_on_device(samp_size, snp_size):
    axes = ("samp", "snp")

    def perm(x, move):
        pairs = []
        for samp in range(samp_size):
            for p in range(snp_size):
                target = move(samp // 2, samp % 2, p)
                if target is None:
                    continue
                tx, tc, tp = target
                if 0 <= tp < snp_size:
                    pairs.append((samp * snp_size + p, (tx * 2 + tc) * snp_size + tp))
        return lax.ppermute(x, axes, pairs)

    def core_swap(x):
        return perm(x, lambda xx, c, p: (xx, 1 - c, p))

    def x_swap(x):
        return perm(x, lambda xx, c, p: (1 - xx, c, p))

    def on_device(genotypes):
        samples, snps = genotypes.shape
        assert samp_size == 4 and snp_size % 2 == 0
        assert snps == 2 * TILE and BAND == 4 * snps
        bf16, f32 = jnp.bfloat16, jnp.float32
        samp = lax.axis_index("samp")
        xx, core = samp // 2, samp % 2
        p = lax.axis_index("snp")
        even = (p % 2) == 0
        first_core = core == 0

        present = (genotypes >= 0).astype(f32)
        dosage = genotypes * present
        stats = jnp.stack([jnp.sum(present, axis=0), jnp.sum(dosage, axis=0), jnp.sum(dosage * dosage, axis=0)])
        stats = stats + core_swap(stats)
        stats = stats + x_swap(stats)
        mine, keep, give = standardize(core[None].astype(jnp.int32), stats, genotypes)

        above = []
        for j in range(CHUNKS):
            above.append(
                (
                    perm(keep[j], lambda xx, c, p: (xx, c, p - 2)),
                    perm(give[j], lambda xx, c, p: (xx, 1 - c, p - 2)),
                )
            )
        up = perm(mine, lambda xx, c, p: (xx, c, p + 2))
        theirs = core_swap(mine)
        rows = (mine, theirs)
        nexts = []
        for j in range(CHUNKS):
            same = perm(
                jnp.where(even, above[j][0], keep[j]), lambda xx, c, p: (xx, c, p + 1) if p % 2 == 0 else (xx, c, p - 1)
            )
            cross = perm(
                jnp.where(even, above[j][1], give[j]),
                lambda xx, c, p: (xx, c, p + 1) if p % 2 == 0 else (xx, 1 - c, p - 1),
            )
            nexts.append((same, cross))
        below = (up, core_swap(up))
        below_low = (below[0][:, TILE:], below[1][:, TILE:])

        own_cols = (
            lax.dynamic_slice_in_dim(mine, core * TILE, TILE, 1),
            lax.dynamic_slice_in_dim(theirs, core * TILE, TILE, 1),
        )
        d0 = dot_pair(rows, own_cols)
        x_d0 = perm(d0.astype(bf16), lambda xx, c, p: (0, c, p) if xx == 1 else None)

        d2 = jnp.concatenate([dot_pair(rows, a) for a in above], axis=1)
        x_d2_top = perm(d2[:TILE].astype(bf16), lambda xx, c, p: (1, c, p) if xx == 0 else None)
        x_d2_low = perm(
            d2[TILE:].astype(bf16), lambda xx, c, p: (1 - xx, c, p) if (xx, c) in ((1, 0), (0, 1)) else None
        )
        d4 = jnp.concatenate([dot_pair(below_low, a).astype(bf16) for a in above], axis=1)
        q_near = perm(d4, lambda xx, c, p: (1, 1, p - 2) if (xx, c) == (1, 0) else None)
        q_far = perm(d4, lambda xx, c, p: (1, 1, p - 2) if (xx, c) == (0, 0) else None)
        d1, x_d1, z_near, z_far = [], [], [], []
        for j in range(CHUNKS):
            part = dot_pair(rows, nexts[j])
            d1.append(part)
            x_d1.append(perm(part.astype(bf16), lambda xx, c, p: (0, c, p) if xx == 1 else None))
            part = dot_pair(below, nexts[j]).astype(bf16)
            z_near.append(perm(part, lambda xx, c, p: (1, c, p - 2) if xx == 1 else None))
            z_far.append(perm(part, lambda xx, c, p: (1, c, p - 2) if xx == 0 else None))

        d0 = d0 + x_d0.astype(f32)
        d1 = jnp.concatenate([a + b.astype(f32) for a, b in zip(d1, x_d1)], axis=1)
        d2_top = d2[:TILE] + x_d2_top.astype(f32)
        d2_low = d2[TILE:] + x_d2_low.astype(f32)
        d3 = jnp.concatenate([a.astype(f32) + b.astype(f32) for a, b in zip(z_near, z_far)], axis=1)
        d4 = q_near.astype(f32) + q_far.astype(f32)

        x_first = xx == 0
        send_top = jnp.where(x_first, jnp.where(first_core, d1[:TILE], d0[:TILE]), jnp.where(first_core, d3[:TILE], d2_top))
        send_low = jnp.where(first_core, jnp.where(x_first, d2_low, 0.0), jnp.where(x_first, d0[TILE:], d2_low))
        got = core_swap(jnp.concatenate([send_top, send_low], axis=0).astype(bf16)).astype(f32)
        own_top = jnp.where(x_first, jnp.where(first_core, d0[:TILE], d1[:TILE]), jnp.where(first_core, d2_top, d3[:TILE]))
        own_low = jnp.where(x_first, d1[TILE:], d3[TILE:])
        got_top = got[:TILE]
        got_low = got[TILE:] + d4
        top = jnp.concatenate(
            [jnp.where(first_core, own_top, got_top), jnp.where(first_core, got_top, own_top)], axis=1
        )
        low = jnp.concatenate(
            [jnp.where(first_core, got_low, own_low), jnp.where(first_core, own_low, got_low)], axis=1
        )
        return jnp.concatenate([top, low], axis=0)

    return on_device


def solution(mesh):
    body = make_on_device(mesh.shape["samp"], mesh.shape["snp"])
    return jax.shard_map(
        body, mesh=mesh, in_specs=(P("samp", "snp"),), out_specs=P("snp", "samp"), check_vma=False
    )
```

```python
import jax
import jax.numpy as jnp
from jax import lax
from jax.sharding import PartitionSpec as P


TILE = 512
BAND = 4096
WIDTH = TILE // 2


def dot_t(rows, cols):
    return lax.dot_general(rows, cols, (((0,), (0,)), ((), ())), preferred_element_type=jnp.float32)


def make_on_device(samp_size, snp_size):
    axes = ("samp", "snp")

    def perm(x, move):
        pairs = []
        for samp in range(samp_size):
            for p in range(snp_size):
                target = move(samp // 2, samp % 2, p)
                if target is None:
                    continue
                tx, tc, tp = target
                if 0 <= tp < snp_size:
                    pairs.append((samp * snp_size + p, (tx * 2 + tc) * snp_size + tp))
        return lax.ppermute(x, axes, pairs)

    def core_swap(x):
        return perm(x, lambda xx, c, p: (xx, 1 - c, p))

    def x_swap(x):
        return perm(x, lambda xx, c, p: (1 - xx, c, p))

    def to_x0(x):
        return perm(x, lambda xx, c, p: (0, c, p) if xx == 1 else None)

    def to_x1(x):
        return perm(x, lambda xx, c, p: (1, c, p) if xx == 0 else None)

    def relay(c, p, crossed):
        return (c, p + 1) if p % 2 == 0 else (1 - c if crossed else c, p - 1)

    def on_device(genotypes):
        _, snps = genotypes.shape
        assert samp_size == 4 and snp_size % 2 == 0
        assert snps == 2 * TILE and BAND == 4 * snps
        bf16, f32 = jnp.bfloat16, jnp.float32
        samp = lax.axis_index("samp")
        xx, core = samp // 2, samp % 2
        x_first, first_core = xx == 0, core == 0
        even = (lax.axis_index("snp") % 2) == 0

        last = [None]

        def after(x):
            return x if last[0] is None else lax.optimization_barrier((x, last[0]))[0]

        def step(make, *args):
            args = (after(args[0]), *args[1:])
            last[0] = make(*args)
            last[0] = lax.optimization_barrier(last[0])
            return last[0]

        present = (genotypes >= 0).astype(f32)
        dosage = genotypes * present
        stats = jnp.stack([jnp.sum(present, axis=0), jnp.sum(dosage, axis=0), jnp.sum(dosage * dosage, axis=0)])
        stats = stats + core_swap(stats)
        stats = stats + x_swap(stats)
        average = stats[1] / stats[0]
        factor = lax.rsqrt(stats[0] * (stats[2] / stats[0] - average * average))
        scale = lax.optimization_barrier(jnp.stack([average, factor]))

        def columns(x, start):
            return lax.dynamic_slice_in_dim(x, start, WIDTH, 1)

        def standardized(by, g):
            return jnp.where(g >= 0, (g - by[0]) * by[1], 0.0).astype(bf16)

        def staged(x):
            return jnp.maximum(x, jnp.finfo(bf16).min)

        def send_same(j):
            return perm(keep[j], lambda xx, c, p: (xx, c, p - 2))

        def send_cross(j):
            return perm(give[j], lambda xx, c, p: (xx, 1 - c, p - 2))

        def relay_same(j):
            payload = step(lambda e: jnp.where(e, above[j][0], keep[j]), even)
            return perm(payload, lambda xx, c, p: (xx, *relay(c, p, False)))

        def relay_cross(j):
            payload = step(lambda e: jnp.where(e, above[j][1], give[j]), even)
            return perm(payload, lambda xx, c, p: (xx, *relay(c, p, True)))

        def pair(rows, cols):
            return step(lambda r: dot_t(r, cols[0]) + dot_t(rows[1], cols[1]), rows[0])

        keep_start, give_start = core * TILE, (1 - core) * TILE
        keep = [step(lambda by: standardized(columns(by, keep_start), columns(genotypes, keep_start)), scale)]
        above = [[send_same(0)]]
        mine = step(standardized, scale, genotypes)
        up = perm(mine, lambda xx, c, p: (xx, c, p + 2))
        theirs = core_swap(mine)
        give = [step(columns, mine, give_start)]
        above[0].append(send_cross(0))
        nexts = [[relay_same(0)]]
        keep.append(step(columns, mine, keep_start + WIDTH))
        above.append([send_same(1)])
        give.append(step(columns, mine, give_start + WIDTH))
        above[1].append(send_cross(1))
        across = [core_swap(give[j]) for j in (0, 1)]
        nexts[0].append(relay_cross(0))
        rows = (mine, step(staged, theirs))
        d0 = [pair(rows, (keep[j], across[j])) for j in (0, 1)]
        x_d0 = to_x0(jnp.concatenate(d0, axis=0).astype(bf16))
        d2 = [pair(rows, above[0])]
        x_d2 = [to_x1(d2[0].astype(bf16))]
        nexts.append([relay_same(1)])
        d1 = [pair(rows, nexts[0])]
        x_d1 = [to_x0(d1[0].astype(bf16))]
        nexts[1].append(relay_cross(1))
        other_up = core_swap(up)
        d2.append(pair(rows, above[1]))
        x_d2.append(to_x1(d2[1].astype(bf16)))
        below = (step(staged, up), step(staged, other_up))
        z_near, z_far = [], []

        def send_d3(j):
            part = pair(below, nexts[j]).astype(bf16)
            z_near.append(perm(part, lambda xx, c, p: (1, c, p - 2) if xx == 1 else None))
            z_far.append(perm(part, lambda xx, c, p: (1, c, p - 2) if xx == 0 else None))

        send_d3(0)
        below_low = (below[0][:, TILE:], below[1][:, TILE:])
        d4 = jnp.concatenate([pair(below_low, a) for a in above], axis=0).astype(bf16)
        q_near = perm(d4, lambda xx, c, p: (1, 1, p - 2) if (xx, c) == (1, 0) else None)
        q_far = perm(d4, lambda xx, c, p: (1, 1, p - 2) if (xx, c) == (0, 0) else None)
        low = jnp.concatenate([d[TILE:] for d in d2], axis=0).astype(bf16)
        x_low = perm(low, lambda xx, c, p: (0, c, p) if (xx, c) == (1, 0) else None)
        send_d3(1)
        d1.append(pair(rows, nexts[1]))
        x_d1.append(to_x0(d1[1].astype(bf16)))

        early, swapped, q_sum = [], [], []
        for j in (0, 1):
            s0 = d0[j] + x_d0[j * snps : (j + 1) * snps].astype(f32)
            s2 = d2[j] + x_d2[j].astype(f32)
            s2_low = d2[j][TILE:] + x_low[j * TILE : (j + 1) * TILE].astype(f32)
            low0, low1 = jnp.where(x_first, s2_low, 0.0), jnp.where(x_first, s0[TILE:], s2[TILE:])
            early.append((jnp.where(x_first, s0[:TILE], s2[:TILE]), jnp.where(first_core, low0, low1)))
            packed = jnp.concatenate(early[j], axis=0).astype(bf16)
            swapped.append(core_swap(packed))
            part = slice(j * TILE, (j + 1) * TILE)
            q_sum.append(q_near[part].astype(f32) + q_far[part].astype(f32))
        out = jnp.zeros((snps, snps), f32)

        def put(out, tile, row, col):
            return lax.dynamic_update_slice(out, tile, (row * TILE, col * WIDTH))

        late, moved = [], []
        for j in (0, 1):
            total = jnp.where(x_first, d1[j] + x_d1[j].astype(f32), z_near[j].astype(f32) + z_far[j].astype(f32))
            late.append(total)
            moved.append(perm(total[:TILE].astype(bf16), lambda xx, c, p: (xx, 1, p) if c == 0 else None))
        for j in (0, 1):
            from_other = swapped[j][TILE:].astype(f32)
            kept_low = jnp.where(first_core, late[j][TILE:], jnp.where(x_first, from_other, q_sum[j]))
            out = put(out, jnp.where(first_core, early[j][0], moved[j].astype(f32)), 0, j)
            out = put(out, jnp.where(first_core, swapped[j][:TILE].astype(f32), late[j][:TILE]), 0, 2 + j)
            out = put(out, jnp.where(first_core, from_other, late[j][TILE:]), 1, j)
            out = put(out, kept_low, 1, 2 + j)
        return out

    return on_device


def solution(mesh):
    body = make_on_device(mesh.shape["samp"], mesh.shape["snp"])

    return jax.shard_map(body, mesh=mesh, in_specs=(P("samp", "snp"),), out_specs=P("snp", "samp"), check_vma=False)
```

```python
import functools

import jax
import jax.numpy as jnp
from jax import lax
from jax.experimental import pallas as pl
from jax.experimental.pallas import tpu as pltpu
from jax.sharding import PartitionSpec as P


TILE = 512
BAND = 4096
WIDTH = TILE // 2


def dot_t(rows, cols):
    return lax.dot_general(rows, cols, (((0,), (0,)), ((), ())), preferred_element_type=jnp.float32)


def merge_body(part, core_ref, keep_top, keep_low, got_top, got_low, *refs):
    out_ref, buffer, wide, sems = refs[-4:]
    core = core_ref[0]

    def put(k, source, row, col):
        start = pl.multiple_of((2 * col + part) * WIDTH, WIDTH)
        return pltpu.make_async_copy(source, out_ref.at[pl.ds(row * TILE, TILE), pl.ds(start, WIDTH)], sems.at[k])

    fetch = pltpu.make_async_copy(got_top, buffer, sems.at[4])
    fetch.start()
    copies = [put(0, keep_top, 0, core), put(1, keep_low, 1, 1 - core), put(2, got_low, 1, core)]
    for copy in copies:
        copy.start()
    fetch.wait()
    wide[...] = buffer[...].astype(jnp.float32)
    last = put(3, wide, 0, 1 - core)
    last.start()
    for copy in copies:
        copy.wait()
    last.wait()


def merge(part, core, tiles, into, columns):
    vmem, anywhere = pl.BlockSpec(memory_space=pltpu.VMEM), pl.BlockSpec(memory_space=pl.ANY)
    tiles = tiles + (() if into is None else (into,))
    return pl.pallas_call(
        functools.partial(merge_body, part),
        grid_spec=pltpu.PrefetchScalarGridSpec(
            num_scalar_prefetch=1,
            grid=(1,),
            in_specs=[vmem, vmem, anywhere, vmem] + [anywhere] * (len(tiles) - 4),
            out_specs=anywhere,
            scratch_shapes=[
                pltpu.VMEM((TILE, WIDTH), jnp.bfloat16),
                pltpu.VMEM((TILE, WIDTH), jnp.float32),
                pltpu.SemaphoreType.DMA((5,)),
            ],
        ),
        out_shape=jax.ShapeDtypeStruct((2 * TILE, columns), jnp.float32),
        input_output_aliases={} if into is None else {5: 0},
        compiler_params=pltpu.CompilerParams(vmem_limit_bytes=8 * 2**20),
        cost_estimate=pl.CostEstimate(flops=TILE * columns, bytes_accessed=4 * TILE * columns, transcendentals=0),
    )(core, *tiles)


def make_on_device(samp_size, snp_size):
    axes = ("samp", "snp")

    def perm(x, move):
        pairs = []
        for samp in range(samp_size):
            for p in range(snp_size):
                target = move(samp // 2, samp % 2, p)
                if target is None:
                    continue
                tx, tc, tp = target
                if 0 <= tp < snp_size:
                    pairs.append((samp * snp_size + p, (tx * 2 + tc) * snp_size + tp))
        return lax.ppermute(x, axes, pairs)

    def core_swap(x):
        return perm(x, lambda xx, c, p: (xx, 1 - c, p))

    def x_swap(x):
        return perm(x, lambda xx, c, p: (1 - xx, c, p))

    def to_x0(x):
        return perm(x, lambda xx, c, p: (0, c, p) if xx == 1 else None)

    def to_x1(x):
        return perm(x, lambda xx, c, p: (1, c, p) if xx == 0 else None)

    def relay(c, p, crossed):
        return (c, p + 1) if p % 2 == 0 else (1 - c if crossed else c, p - 1)

    def on_device(genotypes):
        _, snps = genotypes.shape
        assert samp_size == 4 and snp_size % 2 == 0
        assert snps == 2 * TILE and BAND == 4 * snps
        bf16, f32 = jnp.bfloat16, jnp.float32
        samp = lax.axis_index("samp")
        xx, core = samp // 2, samp % 2
        x_first, first_core = xx == 0, core == 0
        even = (lax.axis_index("snp") % 2) == 0

        last = [None]

        def after(x):
            return x if last[0] is None else lax.optimization_barrier((x, last[0]))[0]

        def step(make, *args):
            args = (after(args[0]), *args[1:])
            last[0] = make(*args)
            last[0] = lax.optimization_barrier(last[0])
            return last[0]

        present = (genotypes >= 0).astype(f32)
        dosage = genotypes * present
        stats = jnp.stack([jnp.sum(present, axis=0), jnp.sum(dosage, axis=0), jnp.sum(dosage * dosage, axis=0)])
        stats = stats + core_swap(stats)
        stats = stats + x_swap(stats)
        average = stats[1] / stats[0]
        factor = lax.rsqrt(stats[0] * (stats[2] / stats[0] - average * average))
        scale = lax.optimization_barrier(jnp.stack([average, factor]))

        def columns(x, start, width=WIDTH):
            return lax.dynamic_slice_in_dim(x, start, width, 1)

        def standardized(by, g):
            return jnp.where(g >= 0, (g - by[0]) * by[1], 0.0).astype(bf16)

        def staged(x):
            return jnp.maximum(x, jnp.finfo(bf16).min)

        def send_same(j):
            return perm(keep[j], lambda xx, c, p: (xx, c, p - 2))

        def send_cross(j):
            return perm(give[j], lambda xx, c, p: (xx, 1 - c, p - 2))

        def relay_same(j):
            payload = step(lambda e: jnp.where(e, above[j][0], keep[j]), even)
            return perm(payload, lambda xx, c, p: (xx, *relay(c, p, False)))

        def relay_cross(j):
            payload = step(lambda e: jnp.where(e, above[j][1], give[j]), even)
            return perm(payload, lambda xx, c, p: (xx, *relay(c, p, True)))

        def pair(rows, cols):
            return step(lambda r: (dot_t(r, cols[0]) + dot_t(rows[1], cols[1])).astype(bf16), rows[0])

        keep_start, give_start = core * TILE, (1 - core) * TILE
        keep = [step(lambda by: standardized(columns(by, keep_start), columns(genotypes, keep_start)), scale)]
        above = [[send_same(0)]]
        mine = step(standardized, scale, genotypes)
        up = perm(mine, lambda xx, c, p: (xx, c, p + 2))
        theirs = core_swap(mine)
        give = [step(columns, mine, give_start)]
        above[0].append(send_cross(0))
        across = core_swap(step(lambda m: columns(m, give_start, TILE), mine))
        nexts = [[relay_same(0)]]
        keep.append(step(columns, mine, keep_start + WIDTH))
        above.append([send_same(1)])
        give.append(step(columns, mine, give_start + WIDTH))
        above[1].append(send_cross(1))
        rows = (mine, step(staged, theirs))
        own = columns(after(mine), keep_start, TILE)
        d0 = pair(rows, (own, across))
        nexts[0].append(relay_cross(0))
        x_d0 = to_x0(d0)


        d2 = [pair(rows, above[0])]
        x_d2 = to_x1(d2[0])
        nexts.append([relay_same(1)])
        d1 = [pair(rows, nexts[0])]
        x_d1 = [to_x0(jnp.concatenate([d1[0], d2[0][TILE:]], axis=0))]
        nexts[1].append(relay_cross(1))
        d2.append(pair(rows, above[1]))
        x_top = to_x1(d2[1][:TILE])
        x_low = perm(d2[1][TILE:], lambda xx, c, p: (1, 1, p) if (xx, c) == (0, 1) else None)
        other_up = core_swap(up)
        below = (step(staged, up), step(staged, other_up))
        z_near, z_far = [], []

        def send_d3(j):
            part = pair(below, nexts[j])
            z_far.append(perm(part, lambda xx, c, p: (1, c, p - 2) if xx == 0 else None))
            z_near.append(perm(part, lambda xx, c, p: (1, c, p - 2) if xx == 1 else None))

        send_d3(0)
        below_low = (below[0][:, TILE:], below[1][:, TILE:])
        d4 = jnp.concatenate([pair(below_low, a) for a in above], axis=0)
        q_near = perm(d4, lambda xx, c, p: (1, 1, p - 2) if (xx, c) == (1, 0) else None)
        q_far = perm(d4, lambda xx, c, p: (1, 1, p - 2) if (xx, c) == (0, 0) else None)
        nexts[1] = [step(staged, n) for n in nexts[1]]
        d1.append(pair(rows, nexts[1]))
        part = jnp.concatenate([d1[1], d2[1][TILE:]], axis=0)
        x_d1.append(to_x0(part))
        send_d3(1)

        core_arg = core[None].astype(jnp.int32)
        out = None
        for j in (0, 1):
            cols = slice(j * WIDTH, (j + 1) * WIDTH)
            s0 = d0[:, cols].astype(f32) + x_d0[:, cols].astype(f32)
            upper, lower = (x_d2[:TILE], x_d2[TILE:]) if j == 0 else (x_top, x_low)
            s2_top = d2[j][:TILE].astype(f32) + upper.astype(f32)
            s2_low = d2[j][TILE:].astype(f32) + jnp.where(x_first, x_d1[j][snps:], lower).astype(f32)
            early_top = jnp.where(x_first, s0[:TILE], s2_top)
            early_low = jnp.where(first_core | ~x_first, s2_low, s0[TILE:])
            late = jnp.where(
                x_first,
                d1[j].astype(f32) + x_d1[j][:snps].astype(f32),
                z_near[j].astype(f32) + z_far[j].astype(f32),
            )
            part = slice(j * TILE, (j + 1) * TILE)
            q_sum = q_near[part].astype(f32) + q_far[part].astype(f32)
            give_top = jnp.where(first_core, late[:TILE], early_top).astype(bf16)
            keep_top = jnp.where(first_core, early_top, late[:TILE])
            send = jnp.concatenate([give_top, early_low.astype(bf16)], axis=0)
            got = core_swap(send)
            got_low = jnp.where(x_first | first_core, got[TILE:].astype(f32), q_sum)
            out = merge(j, core_arg, (keep_top, late[TILE:], got[:TILE], got_low), out, snps)
        return out

    return on_device


def solution(mesh):
    body = make_on_device(mesh.shape["samp"], mesh.shape["snp"])

    return jax.shard_map(body, mesh=mesh, in_specs=(P("samp", "snp"),), out_specs=P("snp", "samp"), check_vma=False)
```

```python
import jax
import jax.numpy as jnp
from jax import lax
from jax.experimental import pallas as pl
from jax.experimental.pallas import tpu as pltpu
from jax.sharding import PartitionSpec as P


TILE = 512
BAND = 4096
WIDTH = TILE // 2


def dot_t(rows, cols):
    return lax.dot_general(rows, cols, (((0,), (0,)), ((), ())), preferred_element_type=jnp.float32)


def merge_body(core_ref, *refs):
    out_ref, buffer, wide, sems = refs[-4:]
    core = core_ref[0]

    def put(k, source, row, col, part):
        start = pl.multiple_of((2 * col + part) * WIDTH, WIDTH)
        return pltpu.make_async_copy(source, out_ref.at[pl.ds(row * TILE, TILE), pl.ds(start, WIDTH)], sems.at[k])

    fetches, copies = [], []
    for part in (0, 1):
        keep_top, keep_low, got_top, got_low = refs[4 * part : 4 * part + 4]
        fetches.append(pltpu.make_async_copy(got_top, buffer.at[part], sems.at[part]))
        copies.append(put(2 + part, keep_top, 0, core, part))
        copies.append(put(4 + part, keep_low, 1, 1 - core, part))
        copies.append(put(6 + part, got_low, 1, core, part))
    for copy in fetches + copies:
        copy.start()
    for part in (0, 1):
        fetches[part].wait()
        wide[part] = buffer[part].astype(jnp.float32)
        last = put(8 + part, wide.at[part], 0, 1 - core, part)
        last.start()
        copies.append(last)
    for copy in copies:
        copy.wait()


def merge(core, tiles, columns):
    vmem, anywhere = pl.BlockSpec(memory_space=pltpu.VMEM), pl.BlockSpec(memory_space=pl.ANY)
    return pl.pallas_call(
        merge_body,
        grid_spec=pltpu.PrefetchScalarGridSpec(
            num_scalar_prefetch=1,
            grid=(1,),
            in_specs=[vmem, vmem, anywhere, vmem] * 2,
            out_specs=anywhere,
            scratch_shapes=[
                pltpu.VMEM((2, TILE, WIDTH), jnp.bfloat16),
                pltpu.VMEM((2, TILE, WIDTH), jnp.float32),
                pltpu.SemaphoreType.DMA((10,)),
            ],
        ),
        out_shape=jax.ShapeDtypeStruct((2 * TILE, columns), jnp.float32),
        compiler_params=pltpu.CompilerParams(vmem_limit_bytes=8 * 2**20),
        cost_estimate=pl.CostEstimate(flops=TILE * columns, bytes_accessed=8 * TILE * columns, transcendentals=0),
    )(core, *tiles)


def make_on_device(samp_size, snp_size):
    axes = ("samp", "snp")

    def perm(x, move):
        pairs = []
        for samp in range(samp_size):
            for p in range(snp_size):
                target = move(samp // 2, samp % 2, p)
                if target is None:
                    continue
                tx, tc, tp = target
                if 0 <= tp < snp_size:
                    pairs.append((samp * snp_size + p, (tx * 2 + tc) * snp_size + tp))
        return lax.ppermute(x, axes, pairs)

    def core_swap(x):
        return perm(x, lambda xx, c, p: (xx, 1 - c, p))

    def x_swap(x):
        return perm(x, lambda xx, c, p: (1 - xx, c, p))

    def to_x0(x):
        return perm(x, lambda xx, c, p: (0, c, p) if xx == 1 else None)

    def to_x1(x):
        return perm(x, lambda xx, c, p: (1, c, p) if xx == 0 else None)

    def relay(c, p, crossed):
        return (c, p + 1) if p % 2 == 0 else (1 - c if crossed else c, p - 1)

    def on_device(genotypes):
        _, snps = genotypes.shape
        assert samp_size == 4 and snp_size % 2 == 0
        assert snps == 2 * TILE and BAND == 4 * snps
        bf16, f32 = jnp.bfloat16, jnp.float32
        samp = lax.axis_index("samp")
        xx, core = samp // 2, samp % 2
        x_first, first_core = xx == 0, core == 0
        even = (lax.axis_index("snp") % 2) == 0

        last = [None]

        def after(x):
            return x if last[0] is None else lax.optimization_barrier((x, last[0]))[0]

        def step(make, *args):
            args = (after(args[0]), *args[1:])
            last[0] = make(*args)
            last[0] = lax.optimization_barrier(last[0])
            return last[0]

        present = (genotypes >= 0).astype(f32)
        dosage = genotypes * present
        stats = jnp.stack([jnp.sum(present, axis=0), jnp.sum(dosage, axis=0), jnp.sum(dosage * dosage, axis=0)])
        stats = x_swap(stats) + perm(stats, lambda xx, c, p: (1 - xx, 1 - c, p)) + (stats + core_swap(stats))
        average = stats[1] / stats[0]
        factor = lax.rsqrt(stats[0] * (stats[2] / stats[0] - average * average))
        scale = lax.optimization_barrier(jnp.stack([average, factor]))

        def columns(x, start, width=WIDTH):
            return lax.dynamic_slice_in_dim(x, start, width, 1)

        def standardized(by, g):
            return jnp.where(g >= 0, (g - by[0]) * by[1], 0.0).astype(bf16)

        def staged(x):
            return jnp.maximum(x, jnp.finfo(bf16).min)

        def send_same(j):
            return perm(keep[j], lambda xx, c, p: (xx, c, p - 2))

        def send_cross(j):
            return perm(give[j], lambda xx, c, p: (xx, 1 - c, p - 2))

        def relay_same(j):
            payload = step(lambda e: jnp.where(e, above[j][0], keep[j]), even)
            return perm(payload, lambda xx, c, p: (xx, *relay(c, p, False)))

        def relay_cross(j):
            payload = step(lambda e: jnp.where(e, above[j][1], give[j]), even)
            return perm(payload, lambda xx, c, p: (xx, *relay(c, p, True)))

        def pair(rows, cols):
            return step(lambda r: (dot_t(r, cols[0]) + dot_t(rows[1], cols[1])).astype(bf16), rows[0])

        keep_start, give_start = core * TILE, (1 - core) * TILE
        keep = [step(lambda by: standardized(columns(by, keep_start), columns(genotypes, keep_start)), scale)]
        above = [[send_same(0)]]
        mine = step(standardized, scale, genotypes)
        up = perm(mine, lambda xx, c, p: (xx, c, p + 2))
        theirs = core_swap(mine)
        give = [step(columns, mine, give_start)]
        above[0].append(send_cross(0))
        across = core_swap(step(lambda m: columns(m, give_start, TILE), mine))
        nexts = [[relay_same(0)]]
        keep.append(step(columns, mine, keep_start + WIDTH))
        above.append([send_same(1)])
        give.append(step(columns, mine, give_start + WIDTH))
        above[1].append(send_cross(1))
        rows = (mine, step(staged, theirs))
        own = columns(after(mine), keep_start, TILE)
        d0 = pair(rows, (own, across))
        nexts[0].append(relay_cross(0))
        x_d0 = to_x0(d0)


        d2 = [pair(rows, above[0])]
        x_d2 = to_x1(d2[0])
        nexts.append([relay_same(1)])
        d1 = [pair(rows, nexts[0])]
        x_d1 = [to_x0(jnp.concatenate([d1[0], d2[0][TILE:]], axis=0))]
        nexts[1].append(relay_cross(1))
        d2.append(pair(rows, above[1]))
        x_top = to_x1(d2[1][:TILE])
        x_low = perm(d2[1][TILE:], lambda xx, c, p: (1, 1, p) if (xx, c) == (0, 1) else None)
        other_up = core_swap(up)
        below = (step(staged, up), step(staged, other_up))
        z_near, z_far = [], []

        def send_d3(j):
            part = pair(below, nexts[j])
            z_far.append(perm(part, lambda xx, c, p: (1, c, p - 2) if xx == 0 else None))
            z_near.append(perm(part, lambda xx, c, p: (1, c, p - 2) if xx == 1 else None))

        send_d3(0)
        below_low = (below[0][:, TILE:], below[1][:, TILE:])
        d4 = jnp.concatenate([pair(below_low, a) for a in above], axis=0)
        q_near = perm(d4, lambda xx, c, p: (1, 1, p - 2) if (xx, c) == (1, 0) else None)
        q_far = perm(d4, lambda xx, c, p: (1, 1, p - 2) if (xx, c) == (0, 0) else None)
        nexts[1] = [step(staged, n) for n in nexts[1]]
        d1.append(pair(rows, nexts[1]))
        part = jnp.concatenate([d1[1], d2[1][TILE:]], axis=0)
        x_d1.append(to_x0(part))
        send_d3(1)

        core_arg = core[None].astype(jnp.int32)
        tiles = []
        for j in (0, 1):
            cols = slice(j * WIDTH, (j + 1) * WIDTH)
            s0 = d0[:, cols].astype(f32) + x_d0[:, cols].astype(f32)
            upper, lower = (x_d2[:TILE], x_d2[TILE:]) if j == 0 else (x_top, x_low)
            s2_top = d2[j][:TILE].astype(f32) + upper.astype(f32)
            s2_low = d2[j][TILE:].astype(f32) + jnp.where(x_first, x_d1[j][snps:], lower).astype(f32)
            early_top = jnp.where(x_first, s0[:TILE], s2_top)
            early_low = jnp.where(first_core | ~x_first, s2_low, s0[TILE:])
            late = jnp.where(
                x_first,
                d1[j].astype(f32) + x_d1[j][:snps].astype(f32),
                z_near[j].astype(f32) + z_far[j].astype(f32),
            )
            part = slice(j * TILE, (j + 1) * TILE)
            q_sum = q_near[part].astype(f32) + q_far[part].astype(f32)
            give_top = jnp.where(first_core, late[:TILE], early_top).astype(bf16)
            keep_top = jnp.where(first_core, early_top, late[:TILE])
            send = jnp.concatenate([give_top, early_low.astype(bf16)], axis=0)
            got = core_swap(send)
            got_low = jnp.where(x_first | first_core, got[TILE:].astype(f32), q_sum)
            tiles += [keep_top, late[TILE:], got[:TILE], got_low]
        return merge(core_arg, tiles, snps)

    return on_device


def solution(mesh):
    body = make_on_device(mesh.shape["samp"], mesh.shape["snp"])

    return jax.shard_map(body, mesh=mesh, in_specs=(P("samp", "snp"),), out_specs=P("snp", "samp"), check_vma=False)
```

```python
import functools

import jax
import jax.numpy as jnp
from jax import lax
from jax.experimental import pallas as pl
from jax.experimental.pallas import tpu as pltpu
from jax.sharding import PartitionSpec as P


TILE = 512
BAND = 4096
WIDTH = TILE // 2


def dot_t(rows, cols):
    return lax.dot_general(rows, cols, (((0,), (0,)), ((), ())), preferred_element_type=jnp.float32)


def merge_body(part, core_ref, keep_top, keep_low, got_top, got_low, *refs):
    out_ref, buffer, wide, sems = refs[-4:]
    core = core_ref[0]

    def put(k, source, row, col):
        start = pl.multiple_of((2 * col + part) * WIDTH, WIDTH)
        return pltpu.make_async_copy(source, out_ref.at[pl.ds(row * TILE, TILE), pl.ds(start, WIDTH)], sems.at[k])

    fetch = pltpu.make_async_copy(got_top, buffer, sems.at[4])
    fetch.start()
    copies = [put(0, keep_top, 0, core), put(1, keep_low, 1, 1 - core), put(2, got_low, 1, core)]
    for copy in copies:
        copy.start()
    fetch.wait()
    wide[...] = buffer[...].astype(jnp.float32)
    last = put(3, wide, 0, 1 - core)
    last.start()
    for copy in copies:
        copy.wait()
    last.wait()


def merge(part, core, tiles, into, columns):
    vmem, anywhere = pl.BlockSpec(memory_space=pltpu.VMEM), pl.BlockSpec(memory_space=pl.ANY)
    tiles = tiles + (() if into is None else (into,))
    return pl.pallas_call(
        functools.partial(merge_body, part),
        grid_spec=pltpu.PrefetchScalarGridSpec(
            num_scalar_prefetch=1,
            grid=(1,),
            in_specs=[vmem, vmem, anywhere, vmem] + [anywhere] * (len(tiles) - 4),
            out_specs=anywhere,
            scratch_shapes=[
                pltpu.VMEM((TILE, WIDTH), jnp.bfloat16),
                pltpu.VMEM((TILE, WIDTH), jnp.float32),
                pltpu.SemaphoreType.DMA((5,)),
            ],
        ),
        out_shape=jax.ShapeDtypeStruct((2 * TILE, columns), jnp.float32),
        input_output_aliases={} if into is None else {5: 0},
        compiler_params=pltpu.CompilerParams(vmem_limit_bytes=8 * 2**20),
        cost_estimate=pl.CostEstimate(flops=TILE * columns, bytes_accessed=4 * TILE * columns, transcendentals=0),
    )(core, *tiles)


def make_on_device(samp_size, snp_size):
    axes = ("samp", "snp")

    def perm(x, move):
        pairs = []
        for samp in range(samp_size):
            for p in range(snp_size):
                target = move(samp // 2, samp % 2, p)
                if target is None:
                    continue
                tx, tc, tp = target
                if 0 <= tp < snp_size:
                    pairs.append((samp * snp_size + p, (tx * 2 + tc) * snp_size + tp))
        return lax.ppermute(x, axes, pairs)

    def core_swap(x):
        return perm(x, lambda xx, c, p: (xx, 1 - c, p))

    def x_swap(x):
        return perm(x, lambda xx, c, p: (1 - xx, c, p))

    def to_x0(x):
        return perm(x, lambda xx, c, p: (0, c, p) if xx == 1 else None)

    def to_x1(x):
        return perm(x, lambda xx, c, p: (1, c, p) if xx == 0 else None)

    def relay(c, p, crossed):
        return (c, p + 1) if p % 2 == 0 else (1 - c if crossed else c, p - 1)

    def on_device(genotypes):
        _, snps = genotypes.shape
        assert samp_size == 4 and snp_size % 2 == 0
        assert snps == 2 * TILE and BAND == 4 * snps
        bf16, f32 = jnp.bfloat16, jnp.float32
        samp = lax.axis_index("samp")
        xx, core = samp // 2, samp % 2
        x_first, first_core = xx == 0, core == 0
        even = (lax.axis_index("snp") % 2) == 0

        last = [None]

        def after(x):
            return x if last[0] is None else lax.optimization_barrier((x, last[0]))[0]

        def step(make, *args):
            args = (after(args[0]), *args[1:])
            last[0] = make(*args)
            last[0] = lax.optimization_barrier(last[0])
            return last[0]

        present = (genotypes >= 0).astype(f32)
        dosage = genotypes * present
        stats = jnp.stack([jnp.sum(present, axis=0), jnp.sum(dosage, axis=0), jnp.sum(dosage * dosage, axis=0)])
        stats = stats + core_swap(stats)
        stats = stats + x_swap(stats)
        average = stats[1] / stats[0]
        factor = lax.rsqrt(stats[0] * (stats[2] / stats[0] - average * average))
        scale = lax.optimization_barrier(jnp.stack([average, factor]))

        def columns(x, start, width=WIDTH):
            return lax.dynamic_slice_in_dim(x, start, width, 1)

        def standardized(by, g):
            return jnp.where(g >= 0, (g - by[0]) * by[1], 0.0).astype(bf16)

        def staged(x):
            return jnp.maximum(x, jnp.finfo(bf16).min)

        def send_same(j):
            return perm(keep[j], lambda xx, c, p: (xx, c, p - 2))

        def send_cross(j):
            return perm(give[j], lambda xx, c, p: (xx, 1 - c, p - 2))

        def relay_same(j):
            payload = step(lambda e: jnp.where(e, above[j][0], keep[j]), even)
            return perm(payload, lambda xx, c, p: (xx, *relay(c, p, False)))

        def relay_cross(j):
            payload = step(lambda e: jnp.where(e, above[j][1], give[j]), even)
            return perm(payload, lambda xx, c, p: (xx, *relay(c, p, True)))

        def pair(rows, cols):
            return step(lambda r: (dot_t(r, cols[0]) + dot_t(rows[1], cols[1])).astype(bf16), rows[0])

        keep_start, give_start = core * TILE, (1 - core) * TILE
        keep = [step(lambda by: standardized(columns(by, keep_start), columns(genotypes, keep_start)), scale)]
        above = [[send_same(0)]]
        mine = step(standardized, scale, genotypes)
        up = perm(mine, lambda xx, c, p: (xx, c, p + 2))
        theirs = core_swap(mine)
        give = [step(columns, mine, give_start)]
        above[0].append(send_cross(0))
        across = core_swap(step(lambda m: columns(m, give_start, TILE), mine))
        nexts = [[relay_same(0)]]
        keep.append(step(columns, mine, keep_start + WIDTH))
        above.append([send_same(1)])
        give.append(step(columns, mine, give_start + WIDTH))
        above[1].append(send_cross(1))
        rows = (mine, step(staged, theirs))
        own = columns(after(mine), keep_start, TILE)
        d0 = pair(rows, (own, across))
        nexts[0].append(relay_cross(0))
        x_d0 = to_x0(d0)


        d2 = [pair(rows, above[0])]
        x_d2 = to_x1(d2[0])
        nexts.append([relay_same(1)])
        d1 = [pair(rows, nexts[0])]
        x_d1 = [to_x0(jnp.concatenate([d1[0], d2[0][TILE:]], axis=0))]
        nexts[1].append(relay_cross(1))
        d2.append(pair(rows, above[1]))
        x_top = to_x1(d2[1][:TILE])
        x_back = perm(d2[1][TILE:], lambda xx, c, p: (0, 0, p) if (xx, c) == (1, 0) else None)
        x_low = perm(d2[1][TILE:], lambda xx, c, p: (1, 1, p) if (xx, c) == (0, 1) else None)
        other_up = core_swap(up)
        below = (step(staged, up), step(staged, other_up))
        z_near, z_far = [], []

        def send_d3(j):
            part = pair(below, nexts[j])
            z_far.append(perm(part, lambda xx, c, p: (1, c, p - 2) if xx == 0 else None))
            z_near.append(perm(part, lambda xx, c, p: (1, c, p - 2) if xx == 1 else None))

        send_d3(0)
        below_low = (below[0][:, TILE:], below[1][:, TILE:])
        d4 = jnp.concatenate([pair(below_low, a) for a in above], axis=0)
        q_near = perm(d4, lambda xx, c, p: (1, 1, p - 2) if (xx, c) == (1, 0) else None)
        q_far = perm(d4, lambda xx, c, p: (1, 1, p - 2) if (xx, c) == (0, 0) else None)
        nexts[1] = [step(staged, n) for n in nexts[1]]
        d1.append(pair(rows, nexts[1]))
        part = d1[1]
        x_d1.append(to_x0(part))
        send_d3(1)

        core_arg = core[None].astype(jnp.int32)
        out = None
        for j in (0, 1):
            cols = slice(j * WIDTH, (j + 1) * WIDTH)
            s0 = d0[:, cols].astype(f32) + x_d0[:, cols].astype(f32)
            upper, lower = (x_d2[:TILE], x_d2[TILE:]) if j == 0 else (x_top, x_low)
            s2_top = d2[j][:TILE].astype(f32) + upper.astype(f32)
            s2_low = d2[j][TILE:].astype(f32) + jnp.where(x_first, x_d1[0][snps:] if j == 0 else x_back, lower).astype(f32)
            early_top = jnp.where(x_first, s0[:TILE], s2_top)
            early_low = jnp.where(first_core | ~x_first, s2_low, s0[TILE:])
            late = jnp.where(
                x_first,
                d1[j].astype(f32) + x_d1[j][:snps].astype(f32),
                z_near[j].astype(f32) + z_far[j].astype(f32),
            )
            part = slice(j * TILE, (j + 1) * TILE)
            q_sum = q_near[part].astype(f32) + q_far[part].astype(f32)
            give_top = jnp.where(first_core, late[:TILE], early_top).astype(bf16)
            keep_top = jnp.where(first_core, early_top, late[:TILE])
            send = jnp.concatenate([give_top, early_low.astype(bf16)], axis=0)
            got = core_swap(send)
            got_low = jnp.where(x_first | first_core, got[TILE:].astype(f32), q_sum)
            out = merge(j, core_arg, (keep_top, late[TILE:], got[:TILE], got_low), out, snps)
        return out

    return on_device


def solution(mesh):
    body = make_on_device(mesh.shape["samp"], mesh.shape["snp"])

    return jax.shard_map(body, mesh=mesh, in_specs=(P("samp", "snp"),), out_specs=P("snp", "samp"), check_vma=False)
```
